32 devices in a mesh: cp: 8 (over y, x, core), tp: 4 (over z).
Axes of the slice: x: 2, y: 2, z: 4, core: 2. Of those that a mesh axis runs over, the one named last changes fastest.
Arguments:
- tokens: bfloat16 [4096, 4096], P('cp'), may hold values from -150 to 150
- gain: bfloat16 [4096], replicated, may hold values from 0.099609375 to 1.8984375
- w_query: bfloat16 [4096, 4096], P(None, 'tp'), may hold values from -3 to 3
- w_key: bfloat16 [4096, 1024], P(None, 'tp'), may hold values from -1 to 1
- w_value: bfloat16 [4096, 1024], P(None, 'tp'), may hold values from -0.09375 to 0.09375
- w_out: bfloat16 [4096, 4096], P('tp'), may hold values from -0.09375 to 0.09375
- doc_ids: int32 [4096], replicated, may hold values from 0 to 7, as said below
Outputs:
- mixed: bfloat16 [4096, 4096], P('cp', 'tp')
The draws below stay inside these ranges and needn't reach their ends.
Inputs may be any that keep to these rules, and one draw needn't show every extreme that they name: `doc_ids`: document numbers never fall along the sequence, and every number of the range is used; every document covers at most 1281 positions; two documents cover exactly 1281, each beginning at the first position of a stretch, one in the first 2048 positions and one starting in the last 2048.
All inputs are finite; a program needn't handle non-finite values.
Results may differ from the reference program's by a relative error of at most 0.015.
Values may be sent and summed in bfloat16 or wider, within the bound.
A program may use at most 128 MiB of HBM per device.

```python
import math
import jax
import jax.numpy as jnp
from jax import lax

D = 4096
HEADS = 32
KV_HEADS = 8
HD = 128
TOK_DEV = 512
REACH = 5
STRETCH = 256
STRETCHES = 16
TOKENS = 4096
DOC_MOST = 1281
DOCS = 8
N_CP = 8
N_TP = 4


def draw_tokens(key, part):
    keys = jax.random.split(jax.random.fold_in(key, 5), 3)
    row_scale = jnp.exp(jax.random.uniform(keys[1], (TOKENS, 1), jnp.float32, 0.0, jnp.log(10.0)))
    col_scale = jnp.exp(jax.random.uniform(keys[2], (1, D), jnp.float32, jnp.log(0.3), jnp.log(3.0)))
    base = jax.random.normal(keys[0], (TOKENS, D), jnp.float32)
    base = jnp.clip(base, -5.0, 5.0)
    return (base * row_scale * col_scale).astype(jnp.bfloat16)


def paired_weights(key):
    keys = jax.random.split(jax.random.fold_in(key, 11), 3)
    fan_scale = D ** (-0.5)
    key_weight = jnp.clip(jax.random.normal(keys[0], (D, KV_HEADS * HD), jnp.float32), -5.0, 5.0) * fan_scale
    query_weight = jnp.clip(jax.random.normal(keys[2], (D, HEADS * HD), jnp.float32), -5.0, 5.0) * fan_scale
    return (jnp.clip(query_weight, -3.0, 3.0), jnp.clip(key_weight, -1.0, 1.0))


def draw_w_query(key, part):
    return paired_weights(key)[0].astype(jnp.bfloat16)


def draw_w_key(key, part):
    return paired_weights(key)[1].astype(jnp.bfloat16)


def draw_doc_ids(key, part):
    keys = jax.random.split(jax.random.fold_in(key, 23), 3)
    first_start = (jax.random.randint(keys[0], (), 1, N_CP // 2 - 1) * STRETCH).astype(jnp.int32)
    second_start = (jax.random.randint(keys[1], (), N_CP, 2 * N_CP - REACH) * STRETCH).astype(jnp.int32)
    places = jnp.arange(TOKENS, dtype=jnp.int32)
    inside_first = (places >= first_start) & (places <= first_start + DOC_MOST)
    inside_second = (places >= second_start) & (places <= second_start + DOC_MOST)
    blocked = inside_first | inside_second | (places == 0)
    ranks = jax.random.permutation(keys[2], TOKENS).astype(jnp.int32)
    scores = jnp.where(blocked, TOKENS + places, ranks).astype(jnp.int32)
    extra_cuts = jnp.argsort(scores, stable=True)[:DOCS - 5].astype(jnp.int32)
    fixed_cuts = jnp.stack([first_start, first_start + DOC_MOST, second_start, second_start + DOC_MOST]).astype(jnp.int32)
    cuts = jnp.concatenate([fixed_cuts, extra_cuts])
    return jnp.sum((places[:, None] >= cuts[None, :]).astype(jnp.int32), axis=1).astype(jnp.int32)


def block_scale(stream_key, extent, shards, low, high):
    loudness = 1.0
    for axis_at, shards_of in shards:
        heights = jax.random.uniform(jax.random.fold_in(jax.random.fold_in(stream_key, 6), axis_at), (shards_of,), jnp.float32, low / len(shards), high / len(shards))
        loudness = loudness * jnp.repeat(jnp.exp(heights), extent[axis_at] // shards_of).reshape((-1,) + (1,) * (len(extent) - 1 - axis_at))
    return loudness


def centred(key, dims, spread, limit, cuts=(), kind=jnp.bfloat16):
    factor_of = block_scale(key, dims, cuts, -0.22, 0.18) if cuts else 1.0
    values = jax.random.normal(key, dims, jnp.float32) * spread * factor_of
    return jnp.minimum(jnp.maximum(values, -limit), limit).astype(kind)


def setup_inputs(seed: int = 0) -> dict:
    splits = jax.random.split(jax.random.key(seed), 8)
    return {
        "tokens": draw_tokens(jax.random.fold_in(splits[7], 71), 0),
        "gain": jnp.clip(1.0 + 0.18 * jax.random.normal(splits[1], (D,), jnp.float32), 0.099609375, 1.8984375).astype(jnp.bfloat16),
        "w_query": draw_w_query(jax.random.fold_in(splits[7], 71), 0),
        "w_key": draw_w_key(jax.random.fold_in(splits[7], 71), 0),
        "w_value": centred(splits[4], (D, KV_HEADS * HD), D ** -0.5, 0.09375, ((1, 4),)),
        "w_out": centred(splits[5], (HEADS * HD, D), (HEADS * HD) ** -0.5, 0.09375, ((0, 4),)),
        "doc_ids": draw_doc_ids(jax.random.fold_in(splits[7], 71), 0),
    }


rope_theta = 500000.0
norm_epsilon = 1e-05
masked_score = -1e+30

def global_positions(row_index, tok_dev, cp_size):
    half_rows = tok_dev // 2
    device = row_index // tok_dev
    within = row_index % tok_dev
    stretch_index = jnp.where(within < half_rows, device, 2 * cp_size - 1 - device)
    return (stretch_index * half_rows + within % half_rows).astype(jnp.int32)

def rotary(heads, positions):
    head_size = heads.shape[-1]
    half_size = head_size // 2
    index = jnp.arange(half_size).astype(jnp.float32)
    freqs = jnp.power(jnp.float32(rope_theta), -2.0 * index / head_size)
    angles = positions.astype(jnp.float32)[:, None] * freqs[None, :]
    cosine = jnp.cos(angles)[:, None, :]
    sine = jnp.sin(angles)[:, None, :]
    lower = heads[..., :half_size]
    upper = heads[..., half_size:]
    return jnp.concatenate([lower * cosine - upper * sine, upper * cosine + lower * sine], axis=-1)

def normalize(tokens, gain):
    widened = tokens.astype(jnp.float32)
    factor = lax.rsqrt(lax.optimization_barrier(jnp.mean(widened * widened, axis=-1, keepdims=True)) + norm_epsilon)
    return (widened * factor * gain.astype(jnp.float32)).astype(jnp.bfloat16)

def reference(tokens, gain, w_query, w_key, w_value, w_out, doc_ids):
    group_size = HEADS // KV_HEADS
    scale = 1.0 / math.sqrt(HD)
    row_index = jnp.arange(TOKENS, dtype=jnp.int32)
    positions = global_positions(row_index, TOK_DEV, N_CP)
    normed = lax.optimization_barrier(normalize(tokens, gain))
    query = jnp.dot(normed, w_query, preferred_element_type=jnp.float32).reshape(TOKENS, HEADS, HD)
    query = lax.optimization_barrier(rotary(query, positions).astype(jnp.bfloat16))
    key_heads = jnp.dot(normed, w_key, preferred_element_type=jnp.float32).reshape(TOKENS, KV_HEADS, HD)
    key_heads = lax.optimization_barrier(rotary(key_heads, positions).astype(jnp.bfloat16))
    value_heads = jnp.dot(normed, w_value, preferred_element_type=jnp.float32).astype(jnp.bfloat16)
    value_heads = lax.optimization_barrier(value_heads).reshape(TOKENS, KV_HEADS, HD)
    order = jnp.zeros((TOKENS,), jnp.int32).at[positions].set(row_index)
    query_seq = query[order]
    pad_rows = REACH * STRETCH
    key_pad = jnp.concatenate([jnp.zeros((pad_rows, KV_HEADS, HD), jnp.bfloat16), key_heads[order]], axis=0)
    value_pad = jnp.concatenate([jnp.zeros((pad_rows, KV_HEADS, HD), jnp.bfloat16), value_heads[order]], axis=0)
    doc_pad = jnp.concatenate([jnp.full((pad_rows,), -1, jnp.int32), doc_ids.astype(jnp.int32)], axis=0)
    span = (REACH + 1) * STRETCH

    def one_stretch(stretch_index):
        start = (stretch_index * STRETCH).astype(jnp.int32)
        query_block = lax.dynamic_slice_in_dim(query_seq, start, STRETCH, 0).astype(jnp.float32)
        query_block = query_block.reshape(STRETCH, KV_HEADS, group_size, HD)
        key_block = lax.dynamic_slice_in_dim(key_pad, start, span, 0).astype(jnp.float32)
        value_block = lax.dynamic_slice_in_dim(value_pad, start, span, 0).astype(jnp.float32)
        query_doc = lax.dynamic_slice_in_dim(doc_ids.astype(jnp.int32), start, STRETCH, 0)
        key_doc = lax.dynamic_slice_in_dim(doc_pad, start, span, 0)
        query_pos = start + jnp.arange(STRETCH, dtype=jnp.int32)
        key_pos = start - pad_rows + jnp.arange(span, dtype=jnp.int32)
        allowed = (key_doc[None, :] == query_doc[:, None]) & (key_pos[None, :] <= query_pos[:, None])
        scores = jnp.einsum('tkgd,skd->kgts', query_block, key_block) * scale
        scores = jnp.where(allowed[None, None], scores, masked_score)
        row_max = lax.optimization_barrier(jnp.max(scores, axis=-1, keepdims=True))
        weights = jnp.where(allowed[None, None], jnp.exp(scores - row_max), 0.0)
        weight_total = lax.optimization_barrier(jnp.sum(weights, axis=-1))
        rounded = lax.optimization_barrier(weights.astype(jnp.bfloat16)).astype(jnp.float32)
        summed = jnp.einsum('kgts,skd->tkgd', rounded, value_block)
        result = summed / jnp.transpose(weight_total, (2, 0, 1))[..., None]
        return result.astype(jnp.bfloat16).reshape(STRETCH, HEADS * HD)
    attention_seq = lax.map(one_stretch, jnp.arange(STRETCHES, dtype=jnp.int32)).reshape(TOKENS, HEADS * HD)
    attention = attention_seq[positions]
    group_cols = HEADS // N_TP * HD
    mixed = jnp.zeros((TOKENS, D), jnp.float32)
    for group_index in range(N_TP):
        low = group_index * group_cols
        partial_value = jnp.dot(attention[:, low:low + group_cols], w_out[low:low + group_cols], preferred_element_type=jnp.float32)
        mixed = mixed + lax.optimization_barrier(partial_value.astype(jnp.bfloat16)).astype(jnp.float32)
    return mixed.astype(jnp.bfloat16)
```

```python
import functools
import math

import jax
import jax.numpy as jnp
from jax import lax
from jax.experimental import pallas as pl
from jax.experimental.pallas import tpu as pltpu
from jax.sharding import PartitionSpec as P

HEADS = 32
KV_HEADS = 8
HD = 128
GROUP = HEADS // KV_HEADS

rope_theta = 500000.0
norm_epsilon = 1e-05
masked_score = -1e30


def normalize(tokens, gain):
    widened = tokens.astype(jnp.float32)
    factor = lax.rsqrt(jnp.mean(widened * widened, axis=-1, keepdims=True) + norm_epsilon)
    return (widened * factor * gain.astype(jnp.float32)).astype(jnp.bfloat16)


def kernel(
    cp, tp, reach,
    normed, cosine, sine, query_doc, key_doc, wq_hbm, wk_hbm, wv_hbm, wo_hbm,
    out,
    wq, wk, wv, wo, query, kv, attn, run_max, run_sum, acc, outbox, from_left, from_right,
    w_sem, kv_send, kv_pass, kv_recv, rs_send, rs_left, rs_right,
):
    tok_dev = normed.shape[0]
    half = tok_dev // 2
    stretches = 2 * cp
    pairs = cp // 2
    kw = wk.shape[1]
    kv_count = kw // HD
    chunks, blocks, rows, width = outbox.shape
    per_half = chunks // 2
    f32 = jnp.float32
    me = lax.axis_index("cp")
    z = lax.axis_index("tp")
    pair = me // 2
    core = me % 2
    sibling = pair * 2 + (1 - core)

    barrier = pltpu.get_barrier_semaphore()
    for step in range(1, cp):
        pl.semaphore_signal(barrier, inc=1, device_id={"cp": lax.rem(me + step, cp)})

    @pl.when(z > 0)
    def _():
        pl.semaphore_signal(barrier, inc=1, device_id={"tp": z - 1})

    @pl.when(z < tp - 1)
    def _():
        pl.semaphore_signal(barrier, inc=1, device_id={"tp": z + 1})

    loads = [
        pltpu.make_async_copy(src, dst, w_sem.at[i])
        for i, (src, dst) in enumerate(((wk_hbm, wk), (wv_hbm, wv), (wq_hbm, wq), (wo_hbm, wo)))
    ]
    for load in loads:
        load.start()

    def needed(target_pair, stretch):
        found = None
        for last in (
            2 * target_pair,
            2 * target_pair + 1,
            stretches - 1 - 2 * target_pair,
            stretches - 2 - 2 * target_pair,
        ):
            hit = jnp.logical_and(stretch <= last, stretch >= last - reach)
            found = hit if found is None else jnp.logical_or(found, hit)
        return found

    def kv_copy(stretch, sem, device):
        return pltpu.make_async_remote_copy(
            src_ref=kv.at[stretch],
            dst_ref=kv.at[stretch],
            send_sem=sem,
            recv_sem=kv_recv.at[stretch],
            device_id={"cp": device},
        )

    def rotate(x, low):
        c = cosine[low : low + x.shape[0], :]
        s = sine[low : low + x.shape[0], :]
        return (x * c + pltpu.roll(x, HD // 2, 1) * s).astype(jnp.bfloat16)

    own = (me, stretches - 1 - me)
    loads[0].wait()
    loads[1].wait()
    for h in (0, 1):
        part = normed[h * half : (h + 1) * half, :]
        keys = jnp.dot(part, wk[...], preferred_element_type=f32)
        for n in range(kv_count):
            kv[own[h], :, n * HD : (n + 1) * HD] = rotate(keys[:, n * HD : (n + 1) * HD], h * half)
        values = jnp.dot(part, wv[...], preferred_element_type=f32)
        kv[own[h], :, kw : 2 * kw] = values.astype(jnp.bfloat16)
        if h == 0:
            count = cp - 1 + (z > 0).astype(jnp.int32) + (z < tp - 1).astype(jnp.int32)
            pl.semaphore_wait(barrier, count)
        for step in range(pairs - 1, 0, -1):
            target = lax.rem(pair + step, pairs)

            @pl.when(needed(target, own[h]))
            def _():
                kv_copy(own[h], kv_send.at[h, step], 2 * target + core).start()

        kv_copy(own[h], kv_send.at[h, 0], sibling).start()

    loads[2].wait()
    tile = 2 * HD

    def query_tile(t, carry):
        low = pl.multiple_of(t * tile, tile)
        raw = jnp.dot(normed[...], wq[:, pl.ds(low, tile)], preferred_element_type=f32)
        query[:, pl.ds(low, tile)] = jnp.concatenate(
            [rotate(raw[:, :HD], 0), rotate(raw[:, HD:], 0)], axis=1
        )
        return carry

    lax.fori_loop(0, wq.shape[1] // tile, query_tile, 0)

    for step in range(1, pairs):
        source = 2 * lax.rem(pair + pairs - step, pairs) + core
        for h, stretch in enumerate((source, stretches - 1 - source)):

            @pl.when(needed(pair, stretch))
            def _():
                kv_copy(stretch, kv_pass.at[h, step], sibling).wait_recv()
                kv_copy(stretch, kv_pass.at[h, step], sibling).start()

    for step in range(pairs):
        source = 2 * lax.rem(pair + pairs - step, pairs) + (1 - core)
        for h, stretch in enumerate((source, stretches - 1 - source)):

            @pl.when(needed(pair, stretch))
            def _():
                kv_copy(stretch, kv_pass.at[h, step], sibling).wait_recv()

    loads[3].wait()
    factor = math.log2(math.e) / math.sqrt(HD)

    def send_right(c, j):
        return pltpu.make_async_remote_copy(
            src_ref=outbox.at[c, j],
            dst_ref=from_left.at[c, j],
            send_sem=rs_send.at[c, j],
            recv_sem=rs_left.at[c, j],
            device_id={"tp": z + 1},
        )

    def send_left(c, j):
        return pltpu.make_async_remote_copy(
            src_ref=outbox.at[c, j],
            dst_ref=from_right.at[c, j],
            send_sem=rs_send.at[c, j],
            recv_sem=rs_right.at[c, j],
            device_id={"tp": z - 1},
        )

    def block_of(t):
        return jnp.where(z < tp // 2, tp - 1 - t, t)

    def attend(c):
        row_low = pl.multiple_of(c * rows, rows)
        last = jnp.where(c < per_half, me, stretches - 1 - me)
        q_pos = last * half + lax.rem(c, per_half) * rows + lax.broadcasted_iota(
            jnp.int32, (rows, 1), 0
        )
        q_doc = query_doc[pl.ds(row_low, rows), :]
        run_max[...] = jnp.full(run_max.shape, masked_score, f32)
        run_sum[...] = jnp.zeros(run_sum.shape, f32)
        acc[...] = jnp.zeros(acc.shape, f32)

        def key_stretch(i, carry):
            s = last - i
            k_pos = s * half + lax.broadcasted_iota(jnp.int32, (1, half), 1)
            allowed = jnp.logical_and(key_doc[s] == q_doc, k_pos <= q_pos)
            for n in range(kv_count):
                heads = jnp.concatenate(
                    [
                        query[pl.ds(row_low, rows), (n * GROUP + g) * HD : (n * GROUP + g + 1) * HD]
                        for g in range(GROUP)
                    ],
                    axis=0,
                )
                scores = lax.dot_general(
                    heads,
                    kv[s, :, n * HD : (n + 1) * HD],
                    (((1,), (1,)), ((), ())),
                    preferred_element_type=f32,
                )
                scores = (scores * factor).reshape(GROUP, rows, half)
                scores = jnp.where(allowed[None], scores, masked_score).reshape(GROUP * rows, half)
                before = run_max[n]
                now = jnp.maximum(before, jnp.max(scores, axis=1, keepdims=True))
                weights = jnp.exp2(scores - now)
                decay = jnp.exp2(before - now)
                run_max[n] = now
                run_sum[n] = run_sum[n] * decay + jnp.sum(weights, axis=1, keepdims=True)
                added = jnp.dot(
                    weights.astype(jnp.bfloat16),
                    kv[s, :, kw + n * HD : kw + (n + 1) * HD],
                    preferred_element_type=f32,
                )
                acc[n] = acc[n] * decay + added
            return carry

        lax.fori_loop(0, jnp.minimum(last, reach) + 1, key_stretch, 0)
        for n in range(kv_count):
            result = (acc[n] / run_sum[n]).astype(jnp.bfloat16)
            for g in range(GROUP):
                attn[:, (n * GROUP + g) * HD : (n * GROUP + g + 1) * HD] = result[
                    g * rows : (g + 1) * rows, :
                ]

    def project(c):
        def one_block(t, carry):
            j = block_of(t)
            low = pl.multiple_of(j * width, width)
            partial = jnp.dot(attn[...], wo[:, pl.ds(low, width)], preferred_element_type=f32)
            outbox[c, j] = partial.astype(jnp.bfloat16)

            @pl.when(jnp.logical_and(z == 0, j > z))
            def _():
                send_right(c, j).start()

            @pl.when(jnp.logical_and(z == tp - 1, j < z))
            def _():
                send_left(c, j).start()

            return carry

        lax.fori_loop(0, blocks, one_block, 0)

    def combine(c):
        def one_block(t, carry):
            j = block_of(t)

            @pl.when(jnp.logical_and(z > 0, j > z))
            def _():
                send_right(c, j).wait_recv()
                total = outbox[c, j].astype(f32) + from_left[c, j].astype(f32)
                outbox[c, j] = total.astype(jnp.bfloat16)
                send_right(c, j).start()

            @pl.when(jnp.logical_and(z < tp - 1, j < z))
            def _():
                send_left(c, j).wait_recv()
                total = outbox[c, j].astype(f32) + from_right[c, j].astype(f32)
                outbox[c, j] = total.astype(jnp.bfloat16)
                send_left(c, j).start()

            return carry

        lax.fori_loop(0, blocks, one_block, 0)

    def one_chunk(c, carry):
        attend(c)
        project(c)

        @pl.when(c > 0)
        def _():
            combine(c - 1)

        return carry

    lax.fori_loop(0, chunks, one_chunk, 0)
    combine(chunks - 1)

    def finish(c, carry):
        @pl.when(z > 0)
        def _():
            send_right(c, z).wait_recv()

        @pl.when(z < tp - 1)
        def _():
            send_left(c, z).wait_recv()

        low = pl.multiple_of(c * rows, rows)

        @pl.when(z == 0)
        def _():
            out[pl.ds(low, rows), :] = (
                outbox[c, z].astype(f32) + from_right[c, z].astype(f32)
            ).astype(jnp.bfloat16)

        @pl.when(z == tp - 1)
        def _():
            out[pl.ds(low, rows), :] = (
                outbox[c, z].astype(f32) + from_left[c, z].astype(f32)
            ).astype(jnp.bfloat16)

        @pl.when(jnp.logical_and(z > 0, z < tp - 1))
        def _():
            out[pl.ds(low, rows), :] = (
                outbox[c, z].astype(f32)
                + from_left[c, z].astype(f32)
                + from_right[c, z].astype(f32)
            ).astype(jnp.bfloat16)

        return carry

    lax.fori_loop(0, chunks, finish, 0)

    for h in (0, 1):
        kv_copy(own[h], kv_send.at[h, 0], sibling).wait_send()
        for step in range(1, pairs):
            target = lax.rem(pair + step, pairs)

            @pl.when(needed(target, own[h]))
            def _():
                kv_copy(own[h], kv_send.at[h, step], 2 * target + core).wait_send()

            source = 2 * lax.rem(pair + pairs - step, pairs) + core
            stretch = source if h == 0 else stretches - 1 - source

            @pl.when(needed(pair, stretch))
            def _():
                kv_copy(stretch, kv_pass.at[h, step], sibling).wait_send()

    def drain(c, carry):
        for j in range(blocks):

            @pl.when(j > z)
            def _():
                send_right(c, j).wait_send()

            @pl.when(j < z)
            def _():
                send_left(c, j).wait_send()

        return carry

    lax.fori_loop(0, chunks, drain, 0)


def shards(cp, tp, tokens, gain, w_query, w_key, w_value, w_out, doc_ids):
    tok_dev, model = tokens.shape
    half = tok_dev // 2
    stretches = 2 * cp
    reach = cp // 2 + 1
    me = lax.axis_index("cp")
    normed = normalize(tokens, gain)
    starts = jnp.stack([me * half, (stretches - 1 - me) * half])
    positions = (starts[:, None] + jnp.arange(half, dtype=jnp.int32)[None, :]).reshape(tok_dev)
    index = jnp.arange(HD // 2).astype(jnp.float32)
    freqs = jnp.power(jnp.float32(rope_theta), -2.0 * index / HD)
    angles = positions.astype(jnp.float32)[:, None] * freqs[None, :]
    cosine = jnp.cos(angles)
    sine = jnp.sin(angles)
    cosine = jnp.concatenate([cosine, cosine], axis=1)
    sine = jnp.concatenate([-sine, sine], axis=1)
    query_doc = jnp.concatenate(
        [
            lax.dynamic_slice_in_dim(doc_ids, me * half, half, 0),
            lax.dynamic_slice_in_dim(doc_ids, (stretches - 1 - me) * half, half, 0),
        ]
    ).reshape(tok_dev, 1)
    key_doc = doc_ids.reshape(stretches, 1, half)

    q_width = w_query.shape[1]
    kw = w_key.shape[1]
    kv_count = kw // HD
    width = model // tp
    chunks = 4
    rows = tok_dev // chunks
    bf16 = jnp.bfloat16
    vmem = pl.BlockSpec(memory_space=pltpu.VMEM)
    hbm = pl.BlockSpec(memory_space=pl.ANY)
    dma = pltpu.SemaphoreType.DMA
    return pl.pallas_call(
        functools.partial(kernel, cp, tp, reach),
        out_shape=jax.ShapeDtypeStruct((tok_dev, width), bf16),
        in_specs=[vmem] * 5 + [hbm] * 4,
        out_specs=vmem,
        scratch_shapes=[
            pltpu.VMEM(w_query.shape, bf16),
            pltpu.VMEM(w_key.shape, bf16),
            pltpu.VMEM(w_value.shape, bf16),
            pltpu.VMEM(w_out.shape, bf16),
            pltpu.VMEM((tok_dev, q_width), bf16),
            pltpu.VMEM((stretches, half, 2 * kw), bf16),
            pltpu.VMEM((rows, q_width), bf16),
            pltpu.VMEM((kv_count, GROUP * rows, 1), jnp.float32),
            pltpu.VMEM((kv_count, GROUP * rows, 1), jnp.float32),
            pltpu.VMEM((kv_count, GROUP * rows, HD), jnp.float32),
            pltpu.VMEM((chunks, tp, rows, width), bf16),
            pltpu.VMEM((chunks, tp, rows, width), bf16),
            pltpu.VMEM((chunks, tp, rows, width), bf16),
            dma((4,)),
            dma((2, cp // 2)),
            dma((2, cp // 2)),
            dma((stretches,)),
            dma((chunks, tp)),
            dma((chunks, tp)),
            dma((chunks, tp)),
        ],
        compiler_params=pltpu.CompilerParams(
            collective_id=0, has_side_effects=True, vmem_limit_bytes=62 * 1024 * 1024
        ),
    )(normed, cosine, sine, query_doc, key_doc, w_query, w_key, w_value, w_out)


def solution(mesh):
    in_specs = (P("cp", None), P(), P(None, "tp"), P(None, "tp"), P(None, "tp"), P("tp", None), P())
    body = functools.partial(shards, mesh.shape["cp"], mesh.shape["tp"])
    return jax.shard_map(
        body, mesh=mesh, in_specs=in_specs, out_specs=P("cp", "tp"), check_vma=False
    )
```

```python
import functools
import math

import jax
import jax.numpy as jnp
import numpy as np
from jax import lax
from jax.experimental import pallas as pl
from jax.experimental.pallas import tpu as pltpu
from jax.sharding import PartitionSpec as P

HEADS = 32
KV_HEADS = 8
HD = 128
GROUP = HEADS // KV_HEADS

rope_theta = 500000.0
norm_epsilon = 1e-05
masked_score = -1e30


def kernel(
    cp, tp, reach,
    gain, inner_cos, inner_sin, base_cos, base_sin, key_doc,
    tokens, wq_hbm, wk_hbm, wv_hbm, wo_hbm,
    out,
    normed, cosine, sine, wq, wk, wv, wo, query, kv, attn, run_max, run_sum, acc, outbox, from_left, from_right,
    t_sem, w_sem, kv_send, kv_pass, kv_recv, rs_send, rs_left, rs_right,
):
    tok_dev = normed.shape[0]
    half = tok_dev // 2
    stretches = 2 * cp
    pairs = cp // 2
    kw = wk.shape[1]
    kv_count = kw // HD
    chunks, blocks, rows, width = outbox.shape
    per_half = chunks // 2
    f32 = jnp.float32
    me = lax.axis_index("cp")
    z = lax.axis_index("tp")
    pair = me // 2
    core = me % 2
    sibling = pair * 2 + (1 - core)

    barrier = pltpu.get_barrier_semaphore()
    for step in range(1, cp):
        pl.semaphore_signal(barrier, inc=1, device_id={"cp": lax.rem(me + step, cp)})

    @pl.when(z > 0)
    def _():
        pl.semaphore_signal(barrier, inc=1, device_id={"tp": z - 1})

    @pl.when(z < tp - 1)
    def _():
        pl.semaphore_signal(barrier, inc=1, device_id={"tp": z + 1})

    own = (me, stretches - 1 - me)
    token_loads = [
        pltpu.make_async_copy(
            tokens.at[pl.ds(h * half, half)], normed.at[pl.ds(h * half, half)], t_sem.at[h]
        )
        for h in (0, 1)
    ]
    loads = [
        pltpu.make_async_copy(src, dst, w_sem.at[i])
        for i, (src, dst) in enumerate(((wk_hbm, wk), (wv_hbm, wv), (wq_hbm, wq), (wo_hbm, wo)))
    ]
    token_loads[0].start()
    loads[0].start()
    loads[1].start()
    token_loads[1].start()
    loads[2].start()
    loads[3].start()

    lane = lax.broadcasted_iota(jnp.int32, (1, HD), 1)
    sign = jnp.where(lane < HD // 2, -1.0, 1.0).astype(f32)
    for h in (0, 1):
        cb = base_cos[pl.ds(own[h], 1), :]
        sb = base_sin[pl.ds(own[h], 1), :]
        cosine[h * half : (h + 1) * half, :] = cb * inner_cos[...] - sb * inner_sin[...]
        sine[h * half : (h + 1) * half, :] = (sign * sb) * inner_cos[...] + (sign * cb) * inner_sin[
            ...
        ]

    def normalize(h):
        step_rows = 16

        def some_rows(i, carry):
            low = pl.multiple_of(h * half + i * step_rows, step_rows)
            wide = normed[pl.ds(low, step_rows), :].astype(f32)
            scale = lax.rsqrt(jnp.mean(wide * wide, axis=1, keepdims=True) + norm_epsilon)
            normed[pl.ds(low, step_rows), :] = (wide * scale * gain[...].astype(f32)).astype(
                jnp.bfloat16
            )
            return carry

        lax.fori_loop(0, half // step_rows, some_rows, 0, unroll=2)

    def within(lasts, stretch):
        found = None
        for last in lasts:
            hit = jnp.logical_and(stretch <= last, stretch >= last - reach)
            found = hit if found is None else jnp.logical_or(found, hit)
        return found

    def needed(target_pair, stretch, phase=None):
        lower = (2 * target_pair, 2 * target_pair + 1)
        upper = (stretches - 1 - lower[0], stretches - 1 - lower[1])
        if phase == 0:
            return within(lower, stretch)
        both = within(lower + upper, stretch)
        if phase is None:
            return both
        return jnp.logical_and(both, jnp.logical_not(within(lower, stretch)))

    def kv_copy(stretch, sem, device):
        return pltpu.make_async_remote_copy(
            src_ref=kv.at[stretch],
            dst_ref=kv.at[stretch],
            send_sem=sem,
            recv_sem=kv_recv.at[stretch],
            device_id={"cp": device},
        )

    def rotate(x, low):
        c = cosine[low : low + x.shape[0], :]
        s = sine[low : low + x.shape[0], :]
        return (x * c + pltpu.roll(x, HD // 2, 1) * s).astype(jnp.bfloat16)

    def keys_values(h):
        part = normed[h * half : (h + 1) * half, :]
        keys = jnp.dot(part, wk[...], preferred_element_type=f32)
        for n in range(kv_count):
            kv[own[h], :, n * HD : (n + 1) * HD] = rotate(keys[:, n * HD : (n + 1) * HD], h * half)
        values = jnp.dot(part, wv[...], preferred_element_type=f32)
        kv[own[h], :, kw : 2 * kw] = values.astype(jnp.bfloat16)

    def send_kv(h, phase):
        for step in range(pairs - 1, 0, -1):
            target = lax.rem(pair + step, pairs)

            @pl.when(needed(target, own[h], phase))
            def _():
                kv_copy(own[h], kv_send.at[h, step], 2 * target + core).start()

    def pass_on(phase):
        for step in range(1, pairs):
            source = 2 * lax.rem(pair + pairs - step, pairs) + core
            for h, stretch in enumerate((source, stretches - 1 - source)):

                @pl.when(needed(pair, stretch, phase))
                def _():
                    kv_copy(stretch, kv_pass.at[h, step], sibling).wait_recv()
                    kv_copy(stretch, kv_pass.at[h, step], sibling).start()

    def await_sibling(phase):
        for step in range(pairs):
            source = 2 * lax.rem(pair + pairs - step, pairs) + (1 - core)
            for h, stretch in enumerate((source, stretches - 1 - source)):

                @pl.when(needed(pair, stretch, phase))
                def _():
                    kv_copy(stretch, kv_pass.at[h, step], sibling).wait_recv()

    def queries(h):
        tile = 2 * HD

        def query_tile(t, carry):
            low = pl.multiple_of(t * tile, tile)
            raw = jnp.dot(
                normed[h * half : (h + 1) * half, :],
                wq[:, pl.ds(low, tile)],
                preferred_element_type=f32,
            )
            query[h * half : (h + 1) * half, pl.ds(low, tile)] = jnp.concatenate(
                [rotate(raw[:, :HD], h * half), rotate(raw[:, HD:], h * half)], axis=1
            )
            return carry

        lax.fori_loop(0, wq.shape[1] // tile, query_tile, 0)

    token_loads[0].wait()
    normalize(0)
    loads[0].wait()
    loads[1].wait()
    keys_values(0)
    count = cp - 1 + (z > 0).astype(jnp.int32) + (z < tp - 1).astype(jnp.int32)
    pl.semaphore_wait(barrier, count)
    send_kv(0, 0)
    kv_copy(own[0], kv_send.at[0, 0], sibling).start()
    token_loads[1].wait()
    normalize(1)
    keys_values(1)
    send_kv(0, 1)
    send_kv(1, None)
    kv_copy(own[1], kv_send.at[1, 0], sibling).start()

    loads[2].wait()
    queries(0)
    pass_on(0)
    await_sibling(0)
    loads[3].wait()
    factor = math.log2(math.e) / math.sqrt(HD)

    def send_right(c, j):
        return pltpu.make_async_remote_copy(
            src_ref=outbox.at[c, j],
            dst_ref=from_left.at[c, j],
            send_sem=rs_send.at[c, j],
            recv_sem=rs_left.at[c, j],
            device_id={"tp": z + 1},
        )

    def send_left(c, j):
        return pltpu.make_async_remote_copy(
            src_ref=outbox.at[c, j],
            dst_ref=from_right.at[c, j],
            send_sem=rs_send.at[c, j],
            recv_sem=rs_right.at[c, j],
            device_id={"tp": z - 1},
        )

    def block_of(t):
        return jnp.where(z < tp // 2, tp - 1 - t, t)

    def attend(c):
        row_low = pl.multiple_of(c * rows, rows)
        last = jnp.where(c < per_half, me, stretches - 1 - me)
        q_pos = last * half + lax.rem(c, per_half) * rows + lax.broadcasted_iota(
            jnp.int32, (rows, 1), 0
        )
        q_docs = key_doc[last * per_half + lax.rem(c, per_half)]
        q_docs = jnp.transpose(jnp.broadcast_to(q_docs, (rows, rows)))
        q_doc = jnp.concatenate([q_docs] * (half // rows), axis=1)
        run_max[...] = jnp.full(run_max.shape, masked_score, f32)
        run_sum[...] = jnp.zeros(run_sum.shape, f32)
        acc[...] = jnp.zeros(acc.shape, f32)

        def key_stretch(i, carry):
            s = last - i
            k_pos = s * half + lax.broadcasted_iota(jnp.int32, (1, half), 1)
            k_doc = jnp.concatenate([key_doc[s * per_half + i] for i in range(per_half)], axis=1)
            allowed = jnp.logical_and(k_doc == q_doc, k_pos <= q_pos)
            for n in range(kv_count):
                heads = jnp.concatenate(
                    [
                        query[pl.ds(row_low, rows), (n * GROUP + g) * HD : (n * GROUP + g + 1) * HD]
                        for g in range(GROUP)
                    ],
                    axis=0,
                )
                scores = lax.dot_general(
                    heads,
                    kv[s, :, n * HD : (n + 1) * HD],
                    (((1,), (1,)), ((), ())),
                    preferred_element_type=f32,
                )
                scores = (scores * factor).reshape(GROUP, rows, half)
                scores = jnp.where(allowed[None], scores, masked_score).reshape(GROUP * rows, half)
                before = run_max[n]
                now = jnp.maximum(before, jnp.max(scores, axis=1, keepdims=True))
                weights = jnp.exp2(scores - now)
                decay = jnp.exp2(before - now)
                run_max[n] = now
                run_sum[n] = run_sum[n] * decay + jnp.sum(weights, axis=1, keepdims=True)
                added = jnp.dot(
                    weights.astype(jnp.bfloat16),
                    kv[s, :, kw + n * HD : kw + (n + 1) * HD],
                    preferred_element_type=f32,
                )
                acc[n] = acc[n] * decay + added
            return carry

        lax.fori_loop(0, jnp.minimum(last, reach) + 1, key_stretch, 0)
        for n in range(kv_count):
            result = (acc[n] / run_sum[n]).astype(jnp.bfloat16)
            for g in range(GROUP):
                attn[:, (n * GROUP + g) * HD : (n * GROUP + g + 1) * HD] = result[
                    g * rows : (g + 1) * rows, :
                ]

    def project(c):
        def one_block(t, carry):
            j = block_of(t)
            low = pl.multiple_of(j * width, width)
            partial = jnp.dot(attn[...], wo[:, pl.ds(low, width)], preferred_element_type=f32)
            outbox[c, j] = partial.astype(jnp.bfloat16)

            @pl.when(jnp.logical_and(z == 0, j > z))
            def _():
                send_right(c, j).start()

            @pl.when(jnp.logical_and(z == tp - 1, j < z))
            def _():
                send_left(c, j).start()

            return carry

        lax.fori_loop(0, blocks, one_block, 0)

    def combine(c):
        def one_block(t, carry):
            j = block_of(t)

            @pl.when(jnp.logical_and(z > 0, j > z))
            def _():
                send_right(c, j).wait_recv()
                total = outbox[c, j].astype(f32) + from_left[c, j].astype(f32)
                outbox[c, j] = total.astype(jnp.bfloat16)
                send_right(c, j).start()

            @pl.when(jnp.logical_and(z < tp - 1, j < z))
            def _():
                send_left(c, j).wait_recv()
                total = outbox[c, j].astype(f32) + from_right[c, j].astype(f32)
                outbox[c, j] = total.astype(jnp.bfloat16)
                send_left(c, j).start()

            return carry

        lax.fori_loop(0, blocks, one_block, 0)

    def one_chunk(c, carry):
        @pl.when(c == per_half)
        def _():
            await_sibling(1)
            queries(1)

        attend(c)
        project(c)

        @pl.when(c == 0)
        def _():
            pass_on(1)

        @pl.when(c > 0)
        def _():
            combine(c - 1)

        return carry

    lax.fori_loop(0, chunks, one_chunk, 0)

    def finish(c, carry):
        @pl.when(z > 0)
        def _():
            send_right(c, z).wait_recv()

        @pl.when(z < tp - 1)
        def _():
            send_left(c, z).wait_recv()

        low = pl.multiple_of(c * rows, rows)

        @pl.when(z == 0)
        def _():
            out[pl.ds(low, rows), :] = (
                outbox[c, z].astype(f32) + from_right[c, z].astype(f32)
            ).astype(jnp.bfloat16)

        @pl.when(z == tp - 1)
        def _():
            out[pl.ds(low, rows), :] = (
                outbox[c, z].astype(f32) + from_left[c, z].astype(f32)
            ).astype(jnp.bfloat16)

        @pl.when(jnp.logical_and(z > 0, z < tp - 1))
        def _():
            out[pl.ds(low, rows), :] = (
                outbox[c, z].astype(f32)
                + from_left[c, z].astype(f32)
                + from_right[c, z].astype(f32)
            ).astype(jnp.bfloat16)

        return carry

    lax.fori_loop(0, chunks - 1, finish, 0)
    combine(chunks - 1)
    finish(chunks - 1, 0)

    for h in (0, 1):
        kv_copy(own[h], kv_send.at[h, 0], sibling).wait_send()
        for step in range(1, pairs):
            target = lax.rem(pair + step, pairs)

            @pl.when(needed(target, own[h]))
            def _():
                kv_copy(own[h], kv_send.at[h, step], 2 * target + core).wait_send()

            source = 2 * lax.rem(pair + pairs - step, pairs) + core
            stretch = source if h == 0 else stretches - 1 - source

            @pl.when(needed(pair, stretch))
            def _():
                kv_copy(stretch, kv_pass.at[h, step], sibling).wait_send()

    def drain(c, carry):
        for j in range(blocks):

            @pl.when(j > z)
            def _():
                send_right(c, j).wait_send()

            @pl.when(j < z)
            def _():
                send_left(c, j).wait_send()

        return carry

    lax.fori_loop(0, chunks, drain, 0)


def shards(cp, tp, tokens, gain, w_query, w_key, w_value, w_out, doc_ids):
    tok_dev, model = tokens.shape
    half = tok_dev // 2
    stretches = 2 * cp
    reach = cp // 2 + 1
    freqs = rope_theta ** (-2.0 * np.arange(HD // 2) / HD)
    freqs = np.concatenate([freqs, freqs])[None, :]
    inner = np.arange(half)[:, None] * freqs
    base = np.arange(stretches)[:, None] * half * freqs
    tables = [f(a).astype(np.float32) for a in (inner, base) for f in (np.cos, np.sin)]

    q_width = w_query.shape[1]
    kw = w_key.shape[1]
    kv_count = kw // HD
    width = model // tp
    rows = half // 2
    chunks = tok_dev // rows
    key_doc = doc_ids.reshape(stretches * half // rows, 1, rows)
    bf16 = jnp.bfloat16
    vmem = pl.BlockSpec(memory_space=pltpu.VMEM)
    hbm = pl.BlockSpec(memory_space=pl.ANY)
    dma = pltpu.SemaphoreType.DMA
    return pl.pallas_call(
        functools.partial(kernel, cp, tp, reach),
        out_shape=jax.ShapeDtypeStruct((tok_dev, width), bf16),
        in_specs=[vmem] * 6 + [hbm] * 5,
        out_specs=vmem,
        scratch_shapes=[
            pltpu.VMEM(tokens.shape, bf16),
            pltpu.VMEM((tok_dev, HD), jnp.float32),
            pltpu.VMEM((tok_dev, HD), jnp.float32),
            pltpu.VMEM(w_query.shape, bf16),
            pltpu.VMEM(w_key.shape, bf16),
            pltpu.VMEM(w_value.shape, bf16),
            pltpu.VMEM(w_out.shape, bf16),
            pltpu.VMEM((tok_dev, q_width), bf16),
            pltpu.VMEM((stretches, half, 2 * kw), bf16),
            pltpu.VMEM((rows, q_width), bf16),
            pltpu.VMEM((kv_count, GROUP * rows, 1), jnp.float32),
            pltpu.VMEM((kv_count, GROUP * rows, 1), jnp.float32),
            pltpu.VMEM((kv_count, GROUP * rows, HD), jnp.float32),
            pltpu.VMEM((chunks, tp, rows, width), bf16),
            pltpu.VMEM((chunks, tp, rows, width), bf16),
            pltpu.VMEM((chunks, tp, rows, width), bf16),
            dma((2,)),
            dma((4,)),
            dma((2, cp // 2)),
            dma((2, cp // 2)),
            dma((stretches,)),
            dma((chunks, tp)),
            dma((chunks, tp)),
            dma((chunks, tp)),
        ],
        compiler_params=pltpu.CompilerParams(
            collective_id=0, has_side_effects=True, vmem_limit_bytes=62 * 1024 * 1024
        ),
    )(gain.reshape(1, model), *tables, key_doc, tokens, w_query, w_key, w_value, w_out)


def solution(mesh):
    in_specs = (P("cp", None), P(), P(None, "tp"), P(None, "tp"), P(None, "tp"), P("tp", None), P())
    body = functools.partial(shards, mesh.shape["cp"], mesh.shape["tp"])
    return jax.shard_map(
        body, mesh=mesh, in_specs=in_specs, out_specs=P("cp", "tp"), check_vma=False
    )
```

```python
import functools
import math

import jax
import jax.numpy as jnp
import numpy as np
from jax import lax
from jax.experimental import pallas as pl
from jax.experimental.pallas import tpu as pltpu
from jax.sharding import PartitionSpec as P

HEADS = 32
KV_HEADS = 8
HD = 128
GROUP = HEADS // KV_HEADS

rope_theta = 500000.0
norm_epsilon = 1e-05
masked_score = -1e30


def kernel(
    cp, tp, reach,
    gain, inner_cos, inner_sin, base_cos, base_sin, key_doc,
    tokens, wq_hbm, wk_hbm, wv_hbm, wo_hbm,
    out,
    normed, cosine, sine, wq, wk, wv, wo, query, kv, key_col, attn, run_max, run_sum, acc, outbox, from_left, from_right,
    t_sem, w_sem, kv_send, kv_pass, kv_recv, rs_send, rs_left, rs_right,
):
    tok_dev = normed.shape[0]
    half = tok_dev // 2
    stretches = 2 * cp
    pairs = cp // 2
    kw = wk.shape[1]
    kv_count = kw // HD
    chunks, blocks, rows, width = outbox.shape
    per_half = chunks // 2
    f32 = jnp.float32
    me = lax.axis_index("cp")
    z = lax.axis_index("tp")
    pair = me // 2
    core = me % 2
    sibling = pair * 2 + (1 - core)

    barrier = pltpu.get_barrier_semaphore()
    for step in range(1, cp):
        pl.semaphore_signal(barrier, inc=1, device_id={"cp": lax.rem(me + step, cp)})

    @pl.when(z > 0)
    def _():
        pl.semaphore_signal(barrier, inc=1, device_id={"tp": z - 1})

    @pl.when(z < tp - 1)
    def _():
        pl.semaphore_signal(barrier, inc=1, device_id={"tp": z + 1})

    own = (me, stretches - 1 - me)
    token_loads = [
        pltpu.make_async_copy(
            tokens.at[pl.ds(h * half, half)], normed.at[pl.ds(h * half, half)], t_sem.at[h]
        )
        for h in (0, 1)
    ]
    loads = [
        pltpu.make_async_copy(src, dst, w_sem.at[i])
        for i, (src, dst) in enumerate(((wk_hbm, wk), (wv_hbm, wv), (wq_hbm, wq), (wo_hbm, wo)))
    ]
    token_loads[0].start()
    loads[0].start()
    loads[1].start()
    token_loads[1].start()
    loads[2].start()
    loads[3].start()

    lane = lax.broadcasted_iota(jnp.int32, (1, HD), 1)
    sign = jnp.where(lane < HD // 2, -1.0, 1.0).astype(f32)
    for h in (0, 1):
        cb = base_cos[pl.ds(own[h], 1), :]
        sb = base_sin[pl.ds(own[h], 1), :]
        cosine[h * half : (h + 1) * half, :] = cb * inner_cos[...] - sb * inner_sin[...]
        sine[h * half : (h + 1) * half, :] = (sign * sb) * inner_cos[...] + (sign * cb) * inner_sin[
            ...
        ]

    def normalize(h):
        step_rows = 16

        def some_rows(i, carry):
            low = pl.multiple_of(h * half + i * step_rows, step_rows)
            wide = normed[pl.ds(low, step_rows), :].astype(f32)
            scale = lax.rsqrt(jnp.mean(wide * wide, axis=1, keepdims=True) + norm_epsilon)
            normed[pl.ds(low, step_rows), :] = (wide * scale * gain[...].astype(f32)).astype(
                jnp.bfloat16
            )
            return carry

        lax.fori_loop(0, half // step_rows, some_rows, 0, unroll=2)

    def within(lasts, stretch):
        found = None
        for last in lasts:
            hit = jnp.logical_and(stretch <= last, stretch >= last - reach)
            found = hit if found is None else jnp.logical_or(found, hit)
        return found

    def needed(target_pair, stretch, phase=None):
        lower = (2 * target_pair, 2 * target_pair + 1)
        upper = (stretches - 1 - lower[0], stretches - 1 - lower[1])
        if phase == 0:
            return within(lower, stretch)
        both = within(lower + upper, stretch)
        if phase is None:
            return both
        return jnp.logical_and(both, jnp.logical_not(within(lower, stretch)))

    def kv_copy(stretch, sem, device):
        return pltpu.make_async_remote_copy(
            src_ref=kv.at[stretch],
            dst_ref=kv.at[stretch],
            send_sem=sem,
            recv_sem=kv_recv.at[stretch],
            device_id={"cp": device},
        )

    def rotate(x, low):
        c = cosine[low : low + x.shape[0], :]
        s = sine[low : low + x.shape[0], :]
        return (x * c + pltpu.roll(x, HD // 2, 1) * s).astype(jnp.bfloat16)

    def keys_values(h):
        part = normed[h * half : (h + 1) * half, :]
        keys = jnp.dot(part, wk[...], preferred_element_type=f32)
        for n in range(kv_count):
            kv[own[h], :, n * HD : (n + 1) * HD] = rotate(keys[:, n * HD : (n + 1) * HD], h * half)
        values = jnp.dot(part, wv[...], preferred_element_type=f32)
        kv[own[h], :, kw : 2 * kw] = values.astype(jnp.bfloat16)

    def send_kv(h, phase):
        for step in range(pairs - 1, 0, -1):
            target = lax.rem(pair + step, pairs)

            @pl.when(needed(target, own[h], phase))
            def _():
                kv_copy(own[h], kv_send.at[h, step], 2 * target + core).start()

    def pass_on(phase):
        for step in range(1, pairs):
            source = 2 * lax.rem(pair + pairs - step, pairs) + core
            for h, stretch in enumerate((source, stretches - 1 - source)):

                @pl.when(needed(pair, stretch, phase))
                def _():
                    kv_copy(stretch, kv_pass.at[h, step], sibling).wait_recv()
                    kv_copy(stretch, kv_pass.at[h, step], sibling).start()

    def await_sibling(phase):
        for step in range(pairs):
            source = 2 * lax.rem(pair + pairs - step, pairs) + (1 - core)
            for h, stretch in enumerate((source, stretches - 1 - source)):

                @pl.when(needed(pair, stretch, phase))
                def _():
                    kv_copy(stretch, kv_pass.at[h, step], sibling).wait_recv()

    def queries(h):
        tile = 2 * HD

        def query_tile(t, carry):
            low = pl.multiple_of(t * tile, tile)
            raw = jnp.dot(
                normed[h * half : (h + 1) * half, :],
                wq[:, pl.ds(low, tile)],
                preferred_element_type=f32,
            )
            query[h * half : (h + 1) * half, pl.ds(low, tile)] = jnp.concatenate(
                [rotate(raw[:, :HD], h * half), rotate(raw[:, HD:], h * half)], axis=1
            )
            return carry

        lax.fori_loop(0, wq.shape[1] // tile, query_tile, 0)

    token_loads[0].wait()
    normalize(0)
    loads[0].wait()
    loads[1].wait()
    keys_values(0)
    count = cp - 1 + (z > 0).astype(jnp.int32) + (z < tp - 1).astype(jnp.int32)
    pl.semaphore_wait(barrier, count)
    send_kv(0, 0)
    kv_copy(own[0], kv_send.at[0, 0], sibling).start()
    token_loads[1].wait()
    normalize(1)
    keys_values(1)
    send_kv(0, 1)
    send_kv(1, None)
    kv_copy(own[1], kv_send.at[1, 0], sibling).start()

    loads[2].wait()
    queries(0)

    def document_column(s, carry):
        for i in range(per_half):
            row = jnp.broadcast_to(key_doc[s * per_half + i], (rows, rows))
            key_col[s, i * rows : (i + 1) * rows, :] = jnp.transpose(row)
        return carry

    lax.fori_loop(0, stretches, document_column, 0)
    pass_on(0)
    await_sibling(0)
    loads[3].wait()
    factor = math.log2(math.e) / math.sqrt(HD)

    def send_right(c, j):
        return pltpu.make_async_remote_copy(
            src_ref=outbox.at[c, j],
            dst_ref=from_left.at[c, j],
            send_sem=rs_send.at[c, j],
            recv_sem=rs_left.at[c, j],
            device_id={"tp": z + 1},
        )

    def send_left(c, j):
        return pltpu.make_async_remote_copy(
            src_ref=outbox.at[c, j],
            dst_ref=from_right.at[c, j],
            send_sem=rs_send.at[c, j],
            recv_sem=rs_right.at[c, j],
            device_id={"tp": z - 1},
        )

    def block_of(t):
        return jnp.where(z < tp // 2, tp - 1 - t, t)

    def attend(c):
        row_low = pl.multiple_of(c * rows, rows)
        last = jnp.where(c < per_half, me, stretches - 1 - me)
        q_pos = last * half + lax.rem(c, per_half) * rows + lax.broadcasted_iota(
            jnp.int32, (1, rows), 1
        )
        q_doc = key_doc[last * per_half + lax.rem(c, per_half)]
        run_max[...] = jnp.full(run_max.shape, masked_score, f32)
        run_sum[...] = jnp.zeros(run_sum.shape, f32)
        acc[...] = jnp.zeros(acc.shape, f32)

        def key_stretch(i, carry):
            s = last - i
            k_pos = s * half + lax.broadcasted_iota(jnp.int32, (half, 1), 0)
            allowed = jnp.logical_and(key_col[s] == q_doc, k_pos <= q_pos)
            for n in range(kv_count):
                heads = jnp.concatenate(
                    [
                        query[pl.ds(row_low, rows), (n * GROUP + g) * HD : (n * GROUP + g + 1) * HD]
                        for g in range(GROUP)
                    ],
                    axis=0,
                )
                scores = lax.dot_general(
                    kv[s, :, n * HD : (n + 1) * HD],
                    heads,
                    (((1,), (1,)), ((), ())),
                    preferred_element_type=f32,
                )
                scores = jnp.concatenate(
                    [
                        jnp.where(allowed, scores[:, g * rows : (g + 1) * rows] * factor, masked_score)
                        for g in range(GROUP)
                    ],
                    axis=1,
                )
                before = run_max[n]
                now = jnp.maximum(before, jnp.max(scores, axis=0, keepdims=True))
                weights = jnp.exp2(scores - now)
                decay = jnp.exp2(before - now)
                run_max[n] = now
                run_sum[n] = run_sum[n] * decay + jnp.sum(weights, axis=0, keepdims=True)
                added = lax.dot_general(
                    kv[s, :, kw + n * HD : kw + (n + 1) * HD],
                    weights.astype(jnp.bfloat16),
                    (((0,), (0,)), ((), ())),
                    preferred_element_type=f32,
                )
                acc[n] = acc[n] * decay + added
            return carry

        lax.fori_loop(0, jnp.minimum(last, reach) + 1, key_stretch, 0)
        for n in range(kv_count):
            result = acc[n] / run_sum[n]
            for g in range(GROUP):
                attn[:, (n * GROUP + g) * HD : (n * GROUP + g + 1) * HD] = jnp.transpose(
                    result[:, g * rows : (g + 1) * rows]
                ).astype(jnp.bfloat16)

    def project(c):
        def one_block(t, carry):
            j = block_of(t)
            low = pl.multiple_of(j * width, width)
            partial = jnp.dot(attn[...], wo[:, pl.ds(low, width)], preferred_element_type=f32)
            outbox[c, j] = partial.astype(jnp.bfloat16)

            @pl.when(jnp.logical_and(z == 0, j > z))
            def _():
                send_right(c, j).start()

            @pl.when(jnp.logical_and(z == tp - 1, j < z))
            def _():
                send_left(c, j).start()

            return carry

        lax.fori_loop(0, blocks, one_block, 0)

    def combine(c):
        def one_block(t, carry):
            j = block_of(t)

            @pl.when(jnp.logical_and(z > 0, j > z))
            def _():
                send_right(c, j).wait_recv()
                total = outbox[c, j].astype(f32) + from_left[c, j].astype(f32)
                outbox[c, j] = total.astype(jnp.bfloat16)
                send_right(c, j).start()

            @pl.when(jnp.logical_and(z < tp - 1, j < z))
            def _():
                send_left(c, j).wait_recv()
                total = outbox[c, j].astype(f32) + from_right[c, j].astype(f32)
                outbox[c, j] = total.astype(jnp.bfloat16)
                send_left(c, j).start()

            return carry

        lax.fori_loop(0, blocks, one_block, 0)

    def one_chunk(c, carry):
        @pl.when(c == per_half)
        def _():
            await_sibling(1)
            queries(1)

        attend(c)
        project(c)

        @pl.when(c == 0)
        def _():
            pass_on(1)

        @pl.when(c > 0)
        def _():
            combine(c - 1)

        return carry

    lax.fori_loop(0, chunks, one_chunk, 0)

    def finish(c, carry):
        @pl.when(z > 0)
        def _():
            send_right(c, z).wait_recv()

        @pl.when(z < tp - 1)
        def _():
            send_left(c, z).wait_recv()

        low = pl.multiple_of(c * rows, rows)

        @pl.when(z == 0)
        def _():
            out[pl.ds(low, rows), :] = (
                outbox[c, z].astype(f32) + from_right[c, z].astype(f32)
            ).astype(jnp.bfloat16)

        @pl.when(z == tp - 1)
        def _():
            out[pl.ds(low, rows), :] = (
                outbox[c, z].astype(f32) + from_left[c, z].astype(f32)
            ).astype(jnp.bfloat16)

        @pl.when(jnp.logical_and(z > 0, z < tp - 1))
        def _():
            out[pl.ds(low, rows), :] = (
                outbox[c, z].astype(f32)
                + from_left[c, z].astype(f32)
                + from_right[c, z].astype(f32)
            ).astype(jnp.bfloat16)

        return carry

    lax.fori_loop(0, chunks - 1, finish, 0)
    combine(chunks - 1)
    finish(chunks - 1, 0)

    for h in (0, 1):
        kv_copy(own[h], kv_send.at[h, 0], sibling).wait_send()
        for step in range(1, pairs):
            target = lax.rem(pair + step, pairs)

            @pl.when(needed(target, own[h]))
            def _():
                kv_copy(own[h], kv_send.at[h, step], 2 * target + core).wait_send()

            source = 2 * lax.rem(pair + pairs - step, pairs) + core
            stretch = source if h == 0 else stretches - 1 - source

            @pl.when(needed(pair, stretch))
            def _():
                kv_copy(stretch, kv_pass.at[h, step], sibling).wait_send()

    def drain(c, carry):
        for j in range(blocks):

            @pl.when(j > z)
            def _():
                send_right(c, j).wait_send()

            @pl.when(j < z)
            def _():
                send_left(c, j).wait_send()

        return carry

    lax.fori_loop(0, chunks, drain, 0)


def shards(cp, tp, tokens, gain, w_query, w_key, w_value, w_out, doc_ids):
    tok_dev, model = tokens.shape
    half = tok_dev // 2
    stretches = 2 * cp
    reach = cp // 2 + 1
    freqs = rope_theta ** (-2.0 * np.arange(HD // 2) / HD)
    freqs = np.concatenate([freqs, freqs])[None, :]
    inner = np.arange(half)[:, None] * freqs
    base = np.arange(stretches)[:, None] * half * freqs
    tables = [f(a).astype(np.float32) for a in (inner, base) for f in (np.cos, np.sin)]

    q_width = w_query.shape[1]
    kw = w_key.shape[1]
    kv_count = kw // HD
    width = model // tp
    rows = half // 2
    chunks = tok_dev // rows
    key_doc = doc_ids.reshape(stretches * half // rows, 1, rows)
    bf16 = jnp.bfloat16
    vmem = pl.BlockSpec(memory_space=pltpu.VMEM)
    hbm = pl.BlockSpec(memory_space=pl.ANY)
    dma = pltpu.SemaphoreType.DMA
    return pl.pallas_call(
        functools.partial(kernel, cp, tp, reach),
        out_shape=jax.ShapeDtypeStruct((tok_dev, width), bf16),
        in_specs=[vmem] * 6 + [hbm] * 5,
        out_specs=vmem,
        scratch_shapes=[
            pltpu.VMEM(tokens.shape, bf16),
            pltpu.VMEM((tok_dev, HD), jnp.float32),
            pltpu.VMEM((tok_dev, HD), jnp.float32),
            pltpu.VMEM(w_query.shape, bf16),
            pltpu.VMEM(w_key.shape, bf16),
            pltpu.VMEM(w_value.shape, bf16),
            pltpu.VMEM(w_out.shape, bf16),
            pltpu.VMEM((tok_dev, q_width), bf16),
            pltpu.VMEM((stretches, half, 2 * kw), bf16),
            pltpu.VMEM((stretches, half, rows), jnp.int32),
            pltpu.VMEM((rows, q_width), bf16),
            pltpu.VMEM((kv_count, 1, GROUP * rows), jnp.float32),
            pltpu.VMEM((kv_count, 1, GROUP * rows), jnp.float32),
            pltpu.VMEM((kv_count, HD, GROUP * rows), jnp.float32),
            pltpu.VMEM((chunks, tp, rows, width), bf16),
            pltpu.VMEM((chunks, tp, rows, width), bf16),
            pltpu.VMEM((chunks, tp, rows, width), bf16),
            dma((2,)),
            dma((4,)),
            dma((2, cp // 2)),
            dma((2, cp // 2)),
            dma((stretches,)),
            dma((chunks, tp)),
            dma((chunks, tp)),
            dma((chunks, tp)),
        ],
        compiler_params=pltpu.CompilerParams(
            collective_id=0, has_side_effects=True, vmem_limit_bytes=62 * 1024 * 1024
        ),
    )(gain.reshape(1, model), *tables, key_doc, tokens, w_query, w_key, w_value, w_out)


def solution(mesh):
    in_specs = (P("cp", None), P(), P(None, "tp"), P(None, "tp"), P(None, "tp"), P("tp", None), P())
    body = functools.partial(shards, mesh.shape["cp"], mesh.shape["tp"])
    return jax.shard_map(
        body, mesh=mesh, in_specs=in_specs, out_specs=P("cp", "tp"), check_vma=False
    )
```
